32 devices in a mesh: dp: 8 (over y, x, core), seq: 4 (over z).
Axes of the slice: x: 2, y: 2, z: 4, core: 2. Of those that a mesh axis runs over, the one named last changes fastest.
Arguments:
- img_q_raw: bfloat16 [8, 512, 1536], P('dp', 'seq'), may hold values from -12 to 12
- img_k_raw: bfloat16 [8, 512, 1536], P('dp', 'seq'), may hold values from -6 to 6
- img_v: bfloat16 [8, 512, 1536], P('dp', 'seq'), may hold values from -6 to 6
- img_dout: bfloat16 [8, 512, 1536], P('dp', 'seq'), may hold values from -6 to 6
- txt_q_raw: bfloat16 [8, 64, 1536], P('dp', 'seq'), may hold values from -6 to 6
- txt_k_raw: bfloat16 [8, 64, 1536], P('dp'), may hold values from -6 to 6
- txt_v: bfloat16 [8, 64, 1536], P('dp'), may hold values from -6 to 6
- txt_dout: bfloat16 [8, 64, 1536], P('dp', 'seq'), may hold values from -6 to 6
- q_gain: float32 [128], replicated, may hold values from 0.6 to 3.8
- k_gain: float32 [128], replicated, may hold values from 0.6 to 3.8
Outputs:
- img_dq: bfloat16 [8, 512, 1536], P('dp', 'seq')
- img_dk: bfloat16 [8, 512, 1536], P('dp', 'seq')
- img_dv: bfloat16 [8, 512, 1536], P('dp', 'seq')
- txt_dq: bfloat16 [8, 64, 1536], P('dp', 'seq')
- txt_dk: bfloat16 [8, 64, 1536], P('dp', 'seq')
- txt_dv: bfloat16 [8, 64, 1536], P('dp', 'seq')
- q_gain_grad: float32 [128], replicated
- k_gain_grad: float32 [128], replicated
The draws below stay inside these ranges and needn't reach their ends.
All inputs are finite; a program needn't handle non-finite values.
Results may differ from the reference program's by a relative error of at most 0.012.
The reference program's roundings to bfloat16 on the way count: a program that leaves them out, or rounds other values in their place, can miss the bound.
Values may be sent and summed in bfloat16 or wider, within the bound.
A program may use at most 64 MiB of HBM per device.

```python
import jax
import jax.numpy as jnp
from jax import lax

HEADS = 12
HEAD_DIM = 128
IMG_DEV = 128
TEXT = 64
IMAGE = 512
BATCH = 8
N_SEQ = 4


def joint_image(key):
    base = jax.random.fold_in(key, 7)
    first_key, second_key = jax.random.split(base, 2)
    keys_image = jnp.clip(jax.random.normal(first_key, (BATCH, IMAGE, HEADS * HEAD_DIM), jnp.float32), -6.0, 6.0)
    queries = jnp.clip(jax.random.normal(second_key, (BATCH, IMAGE, HEADS * HEAD_DIM), jnp.float32), -6.0, 6.0)
    return (queries, keys_image)


def draw_img_q_raw(key, part):
    return joint_image(key)[0].astype(jnp.bfloat16)


def draw_img_k_raw(key, part):
    return joint_image(key)[1].astype(jnp.bfloat16)


def draw_q_gain(key, part):
    base = jax.random.fold_in(key, 11)
    return jax.random.uniform(base, (HEAD_DIM,), jnp.float32, 0.6, 1.4)


def draw_k_gain(key, part):
    base = jax.random.fold_in(key, 13)
    return jax.random.uniform(base, (HEAD_DIM,), jnp.float32, 0.6, 1.4)


def steps_of(key, shape, pieces, least, high):
    def one(dim, parts):
        heights = jax.random.uniform(jax.random.fold_in(jax.random.fold_in(key, 6), dim), (parts,), jnp.float32, least / len(pieces), high / len(pieces))
        return jnp.repeat(jnp.exp(heights), shape[dim] // parts).reshape((-1,) + (1,) * (len(shape) - dim - 1))

    factor_of = one(*pieces[0])
    for cut in pieces[1:]:
        factor_of = factor_of * one(*cut)
    return factor_of


def gaussian(key, extent, deviation, most, cuts=(), dtype=jnp.bfloat16):
    factor_of = steps_of(key, extent, cuts, -0.22, 0.18) if cuts else 1.0
    array = jax.random.normal(key, extent, jnp.float32) * deviation * factor_of
    return jnp.minimum(jnp.maximum(array, -most), most).astype(dtype)


def setup_inputs(seed: int = 0) -> dict:
    splits = jax.random.split(jax.random.key(seed), 11)
    return {
        "img_q_raw": draw_img_q_raw(jax.random.fold_in(splits[10], 71), 0),
        "img_k_raw": draw_img_k_raw(jax.random.fold_in(splits[10], 71), 0),
        "img_v": gaussian(splits[2], (BATCH, IMAGE, HEADS * HEAD_DIM), 1.0, 6.0, ((0, 8), (1, 4))),
        "img_dout": gaussian(splits[3], (BATCH, IMAGE, HEADS * HEAD_DIM), 1.0, 6.0, ((0, 8), (1, 4))),
        "txt_q_raw": gaussian(splits[4], (BATCH, TEXT, HEADS * HEAD_DIM), 1.0, 6.0, ((0, 8), (1, 4))),
        "txt_k_raw": gaussian(splits[5], (BATCH, TEXT, HEADS * HEAD_DIM), 1.0, 6.0, ((0, 8),)),
        "txt_v": gaussian(splits[6], (BATCH, TEXT, HEADS * HEAD_DIM), 1.0, 6.0, ((0, 8),)),
        "txt_dout": gaussian(splits[7], (BATCH, TEXT, HEADS * HEAD_DIM), 1.0, 6.0, ((0, 8), (1, 4))),
        "q_gain": draw_q_gain(jax.random.fold_in(splits[10], 71), 0),
        "k_gain": draw_k_gain(jax.random.fold_in(splits[10], 71), 0),
    }


epsilon = 1e-06

def normalize(source, norm_gain):
    values = source.astype(jnp.float32)
    inverse = lax.rsqrt(lax.optimization_barrier(jnp.mean(values * values, axis=-1, keepdims=True)) + epsilon)
    return values * inverse * norm_gain

def rounded(values):
    return lax.optimization_barrier(values.astype(jnp.bfloat16)).astype(jnp.float32)

def blocked(image_rows, text_rows):
    image_part = image_rows.reshape(N_SEQ, IMG_DEV, HEADS, HEAD_DIM)
    text_part = text_rows.reshape(N_SEQ, TEXT // N_SEQ, HEADS, HEAD_DIM)
    return jnp.concatenate([image_part, text_part], axis=1)

def sample(q_gain, k_gain, inputs):
    img_q, img_k, img_val, img_grad, txt_q, txt_k, txt_val, txt_grad = inputs
    query_src = blocked(img_q, txt_q).astype(jnp.float32)
    dout_f = blocked(img_grad, txt_grad).astype(jnp.float32)
    key_src = jnp.concatenate([img_k, txt_k], axis=0).reshape(IMAGE + TEXT, HEADS, HEAD_DIM).astype(jnp.float32)
    value_all = jnp.concatenate([img_val, txt_val], axis=0).reshape(IMAGE + TEXT, HEADS, HEAD_DIM).astype(jnp.float32)
    query_b = rounded(normalize(query_src, q_gain))
    key_b = rounded(normalize(key_src, k_gain))
    score_scale = HEAD_DIM ** (-0.5)
    scores = jnp.einsum('nqhd,khd->nhqk', query_b, key_b) * score_scale
    row_max = lax.optimization_barrier(jnp.max(scores, axis=-1, keepdims=True))
    shifted = scores - row_max
    log_total = jnp.log(lax.optimization_barrier(jnp.sum(jnp.exp(shifted), axis=-1, keepdims=True)))
    prob_full = jnp.exp(shifted - log_total)
    probs_b = rounded(prob_full)
    output_b = rounded(jnp.einsum('nhqk,khd->nqhd', probs_b, value_all))
    dprob = jnp.einsum('nqhd,khd->nhqk', dout_f, value_all)
    row_delta = jnp.transpose(lax.optimization_barrier(jnp.sum(dout_f * output_b, axis=-1)), (0, 2, 1))[..., None]
    dscore_b = rounded(prob_full * (dprob - row_delta) * score_scale)
    dquery = jnp.einsum('nhqk,khd->nqhd', dscore_b, key_b)
    dkey = lax.optimization_barrier(jnp.sum(rounded(jnp.einsum('nhqk,nqhd->nkhd', dscore_b, query_b)), axis=0))
    dvalue = lax.optimization_barrier(jnp.sum(rounded(jnp.einsum('nhqk,nqhd->nkhd', probs_b, dout_f)), axis=0))
    result_q, query_pull = jax.vjp(normalize, query_src, q_gain)
    dquery_src, dq_gain = query_pull(dquery)
    result_k, key_pull = jax.vjp(normalize, key_src, k_gain)
    dkey_src, dk_gain = key_pull(dkey)
    width_all = HEADS * HEAD_DIM
    dq_b = dquery_src.astype(jnp.bfloat16)
    image_dq = dq_b[:, :IMG_DEV].reshape(IMAGE, width_all)
    text_dq = dq_b[:, IMG_DEV:].reshape(TEXT, width_all)
    dk_b = dkey_src.reshape(IMAGE + TEXT, width_all).astype(jnp.bfloat16)
    dv_b = dvalue.reshape(IMAGE + TEXT, width_all).astype(jnp.bfloat16)
    return (image_dq, dk_b[:IMAGE], dv_b[:IMAGE], text_dq, dk_b[IMAGE:], dv_b[IMAGE:], dq_gain, dk_gain)

def reference(img_q_raw, img_k_raw, img_v, img_dout, txt_q_raw, txt_k_raw, txt_v, txt_dout, q_gain, k_gain):

    def per_sample(inputs):
        return sample(q_gain, k_gain, inputs)
    results = lax.map(per_sample, (img_q_raw, img_k_raw, img_v, img_dout, txt_q_raw, txt_k_raw, txt_v, txt_dout))
    return (results[0], results[1], results[2], results[3], results[4], results[5], lax.optimization_barrier(jnp.sum(results[6], axis=0)), lax.optimization_barrier(jnp.sum(results[7], axis=0)))
```

```python
import functools

import jax
import jax.numpy as jnp
from jax import lax
from jax.experimental import pallas as pl
from jax.experimental.pallas import tpu as pltpu
from jax.sharding import PartitionSpec as P

MESH = pl.DeviceIdType.MESH
HEAD_DIM = 128
EPSILON = 1e-06
F32 = jnp.float32
BF16 = jnp.bfloat16


def dot(a, b, contract):
    return lax.dot_general(a, b, ((contract[:1], contract[1:]), ((), ())), preferred_element_type=F32)


def inverse_rms(values):
    return lax.rsqrt(jnp.mean(values * values, axis=-1, keepdims=True) + EPSILON)


def norm_back(values, inverse, gain, upstream):
    unit = values * inverse
    lifted = upstream * gain
    mean = jnp.mean(lifted * unit, axis=-1, keepdims=True)
    return inverse * (lifted - unit * mean), upstream * unit


def partners(me, n):
    if n == 4:
        return [lax.rem(me + 2, n), 3 - me, me + 1 - 2 * lax.rem(me, 2)]
    return [lax.rem(me + step, n) for step in range(1, n)]


def kernel(
    n, dp, heads,
    iq, ik, iv, idt, tq, tk, tv, td, q_gain, k_gain,
    o_iq, o_ik, o_iv, o_tq, o_tk, o_tv, o_gain,
    qbuf, kbuf, vbuf, dbuf, knb, dka, dva, gq, gk, gv, gsum, dpbuf, sqbuf,
    fs, fr, bs, br, ls, gs, gr,
):
    me = lax.axis_index("seq")
    my_dp = lax.axis_index("dp")
    img, txt, text = iq.shape[0], tq.shape[0], tk.shape[0]
    block = img + txt
    image = img * n
    others = partners(me, n)

    def col(owner, h):
        return pl.ds(pl.multiple_of((owner * heads + h) * HEAD_DIM, HEAD_DIM), HEAD_DIM)

    def rows(start, size, unit):
        return pl.ds(pl.multiple_of(start, unit), size)

    barrier = pltpu.get_barrier_semaphore()
    for other in others:
        pl.semaphore_signal(barrier, inc=1, device_id={"seq": other}, device_id_type=MESH)

    def greet(step, carry):
        pl.semaphore_signal(
            barrier, inc=1, device_id={"dp": lax.rem(my_dp + step, dp)}, device_id_type=MESH
        )
        return carry

    lax.fori_loop(1, dp, greet, 0)
    pl.semaphore_wait(barrier, n - 1 + dp - 1)

    def forward_parts(h, source):
        return (
            (iq, qbuf.at[h, rows(source * block, img, 16)]),
            (ik, kbuf.at[h, rows(source * img, img, 16)]),
            (iv, vbuf.at[h, rows(source * img, img, 16)]),
            (idt, dbuf.at[h, rows(source * block, img, 16)]),
            (tq, qbuf.at[h, rows(source * block + img, txt, 16)]),
            (td, dbuf.at[h, rows(source * block + img, txt, 16)]),
        )

    def forward_copy(part, h, source, target):
        src, dst = forward_parts(h, source)[part]
        return pltpu.make_async_remote_copy(
            src_ref=src.at[:, col(target, h)], dst_ref=dst,
            send_sem=fs.at[part, h, target], recv_sem=fr.at[part, h, source],
            device_id={"seq": target}, device_id_type=MESH,
        )

    def send_head(h, carry):
        for other in others:
            for part in range(6):
                forward_copy(part, h, me, other).start()
        return carry

    lax.fori_loop(0, heads, send_head, 0)

    def own_head(h, carry):
        for src, dst in forward_parts(h, me):
            dst[...] = src[:, col(me, h)]
        kbuf[h, image:image + text] = tk[:, col(me, h)]
        vbuf[h, image:image + text] = tv[:, col(me, h)]
        return carry

    lax.fori_loop(0, heads, own_head, 0)
    gsum[...] = jnp.zeros_like(gsum)

    def back_parts(h, target):
        return (
            (gq.at[h, rows(target * block, img, 16)], o_iq),
            (gk.at[h, rows(target * img, img, 16)], o_ik),
            (gv.at[h, rows(target * img, img, 16)], o_iv),
            (gq.at[h, rows(target * block + img, txt, 16)], o_tq),
            (gk.at[h, rows(image + target * txt, txt, 16)], o_tk),
            (gv.at[h, rows(image + target * txt, txt, 16)], o_tv),
        )

    def back_copy(part, h, source, target):
        src, dst = back_parts(h, target)[part]
        return pltpu.make_async_remote_copy(
            src_ref=src, dst_ref=dst.at[:, col(source, h)],
            send_sem=bs.at[part, h, target], recv_sem=br.at[part, h, source],
            device_id={"seq": target}, device_id_type=MESH,
        )

    qg = q_gain[...]
    kg = k_gain[...]
    scale = HEAD_DIM ** (-0.5)

    def head(h, carry):
        for other in others:
            for part in range(6):
                forward_copy(part, h, other, me).wait_recv()
        key_src = kbuf[h].astype(F32)
        key_inv = inverse_rms(key_src)
        knb[...] = (key_src * key_inv * kg).astype(BF16)
        dka[...] = jnp.zeros_like(dka)
        dva[...] = jnp.zeros_like(dva)

        def one_block(j, inner):
            here = rows(j * block, block, 16)
            query_src = qbuf[h, here].astype(F32)
            query_inv = inverse_rms(query_src)
            qn = (query_src * query_inv * qg).astype(BF16)
            kn = knb[...]
            value = vbuf[h]
            dout = dbuf[h, here]
            scores = dot(qn, kn, (1, 1)) * scale
            exps = jnp.exp(scores - jnp.max(scores, axis=-1, keepdims=True))
            prob = exps * (1.0 / jnp.sum(exps, axis=-1, keepdims=True))
            prob_b = prob.astype(BF16)
            output = dot(prob_b, value, (1, 0)).astype(BF16)
            dprob = dot(dout, value, (1, 1))
            delta = jnp.sum(dout.astype(F32) * output.astype(F32), axis=-1, keepdims=True)
            dscore = (prob * (dprob - delta) * scale).astype(BF16)
            dqn = dot(dscore, kn, (1, 0))
            dka[...] += dot(dscore, qn, (0, 0)).astype(BF16).astype(F32)
            dva[...] += dot(prob_b, dout, (0, 0)).astype(BF16).astype(F32)
            dq, term = norm_back(query_src, query_inv, qg, dqn)
            gq[h, here] = dq.astype(BF16)
            gsum[0:1, :] += jnp.sum(term, axis=0, keepdims=True)
            return inner

        lax.fori_loop(0, n, one_block, 0)
        gv[h] = dva[...].astype(BF16)
        dk, term = norm_back(key_src, key_inv, kg, dka[...])
        gk[h] = dk.astype(BF16)
        gsum[1:2, :] += jnp.sum(term, axis=0, keepdims=True)
        for other in others:
            for part in range(6):
                back_copy(part, h, me, other).start()
        for part, (src, dst) in enumerate(back_parts(h, me)):
            pltpu.make_async_copy(src, dst.at[:, col(me, h)], ls.at[part, h]).start()
        return carry

    lax.fori_loop(0, heads, head, 0)

    dpbuf[my_dp] = gsum[...]

    def dp_copy(target):
        return pltpu.make_async_remote_copy(
            src_ref=dpbuf.at[my_dp], dst_ref=dpbuf.at[my_dp], send_sem=gs.at[0], recv_sem=gr.at[0],
            device_id={"dp": target}, device_id_type=MESH,
        )

    def dp_send(step, carry):
        dp_copy(lax.rem(my_dp + step, dp)).start()
        return carry

    lax.fori_loop(1, dp, dp_send, 0)
    rest = dpbuf.at[pl.ds(0, dp - 1)]
    pltpu.make_async_copy(rest, rest, gr.at[0]).wait()
    pltpu.make_async_copy(rest, rest, gs.at[0]).wait()
    sqbuf[me] = jnp.sum(dpbuf[...], axis=0)
    for other in others:
        pltpu.make_async_remote_copy(
            src_ref=sqbuf.at[me], dst_ref=sqbuf.at[me], send_sem=gs.at[1], recv_sem=gr.at[1],
            device_id={"seq": other}, device_id_type=MESH,
        ).start()

    def drain(h, carry):
        for part, (src, dst) in enumerate(back_parts(h, me)):
            pltpu.make_async_copy(src, dst.at[:, col(me, h)], ls.at[part, h]).wait()
        for other in others:
            for part in range(6):
                forward_copy(part, h, me, other).wait_send()
                back_copy(part, h, me, other).wait_send()
                back_copy(part, h, other, me).wait_recv()
        return carry

    lax.fori_loop(0, heads, drain, 0)
    rest = sqbuf.at[pl.ds(0, n - 1)]
    pltpu.make_async_copy(rest, rest, gr.at[1]).wait()
    pltpu.make_async_copy(rest, rest, gs.at[1]).wait()
    o_gain[...] = jnp.sum(sqbuf[...], axis=0)


def local(n, dp, iq, ik, iv, idt, tq, tk, tv, td, q_gain, k_gain):
    img, width = iq.shape[1:]
    txt, text = tq.shape[1], tk.shape[1]
    heads = width // HEAD_DIM // n
    keys = img * n + text
    queries = (img + txt) * n
    vmem = pl.BlockSpec(memory_space=pltpu.VMEM)
    out = pl.pallas_call(
        functools.partial(kernel, n, dp, heads),
        out_shape=(
            jax.ShapeDtypeStruct((img, width), BF16),
            jax.ShapeDtypeStruct((img, width), BF16),
            jax.ShapeDtypeStruct((img, width), BF16),
            jax.ShapeDtypeStruct((txt, width), BF16),
            jax.ShapeDtypeStruct((txt, width), BF16),
            jax.ShapeDtypeStruct((txt, width), BF16),
            jax.ShapeDtypeStruct((2, HEAD_DIM), F32),
        ),
        in_specs=[vmem] * 10,
        out_specs=(vmem,) * 7,
        scratch_shapes=[
            pltpu.VMEM((heads, queries, HEAD_DIM), BF16),
            pltpu.VMEM((heads, keys, HEAD_DIM), BF16),
            pltpu.VMEM((heads, keys, HEAD_DIM), BF16),
            pltpu.VMEM((heads, queries, HEAD_DIM), BF16),
            pltpu.VMEM((keys, HEAD_DIM), BF16),
            pltpu.VMEM((keys, HEAD_DIM), F32),
            pltpu.VMEM((keys, HEAD_DIM), F32),
            pltpu.VMEM((heads, queries, HEAD_DIM), BF16),
            pltpu.VMEM((heads, keys, HEAD_DIM), BF16),
            pltpu.VMEM((heads, keys, HEAD_DIM), BF16),
            pltpu.VMEM((2, HEAD_DIM), F32),
            pltpu.VMEM((dp, 2, HEAD_DIM), F32),
            pltpu.VMEM((n, 2, HEAD_DIM), F32),
            pltpu.SemaphoreType.DMA((6, heads, n)),
            pltpu.SemaphoreType.DMA((6, heads, n)),
            pltpu.SemaphoreType.DMA((6, heads, n)),
            pltpu.SemaphoreType.DMA((6, heads, n)),
            pltpu.SemaphoreType.DMA((6, heads)),
            pltpu.SemaphoreType.DMA((2,)),
            pltpu.SemaphoreType.DMA((2,)),
        ],
        compiler_params=pltpu.CompilerParams(collective_id=0, has_side_effects=True),
    )(
        iq[0], ik[0], iv[0], idt[0], tq[0], tk[0], tv[0], td[0],
        q_gain.reshape(1, HEAD_DIM), k_gain.reshape(1, HEAD_DIM),
    )
    return (*(grad[None] for grad in out[:6]), out[6][0], out[6][1])


def solution(mesh):
    split = P("dp", "seq", None)
    whole = P("dp", None, None)
    return jax.shard_map(
        functools.partial(local, mesh.shape["seq"], mesh.shape["dp"]),
        mesh=mesh,
        in_specs=(split, split, split, split, split, whole, whole, split, P(), P()),
        out_specs=(split,) * 6 + (P(), P()),
        check_vma=False,
    )
```

```python
import functools

import jax
import jax.numpy as jnp
from jax import lax
from jax.experimental import pallas as pl
from jax.experimental.pallas import tpu as pltpu
from jax.sharding import PartitionSpec as P

MESH = pl.DeviceIdType.MESH
HEAD_DIM = 128
EPSILON = 1e-06
F32 = jnp.float32
BF16 = jnp.bfloat16


def dot(a, b, contract):
    return lax.dot_general(a, b, ((contract[:1], contract[1:]), ((), ())), preferred_element_type=F32)


def inverse_rms(values):
    return lax.rsqrt(jnp.mean(values * values, axis=-1, keepdims=True) + EPSILON)


def norm_back(values, inverse, gain, upstream):
    unit = values * inverse
    lifted = upstream * gain
    mean = jnp.mean(lifted * unit, axis=-1, keepdims=True)
    return inverse * (lifted - unit * mean), upstream * unit


def partners(me, n):
    if n == 4:
        return [lax.rem(me + 2, n), 3 - me, me + 1 - 2 * lax.rem(me, 2)]
    return [lax.rem(me + step, n) for step in range(1, n)]


def kernel(
    n, dp, heads,
    h_iq, h_ik, h_iv, h_idt, h_tq, h_tk, h_tv, h_td, q_gain, k_gain,
    o_iq, o_ik, o_iv, o_tq, o_tk, o_tv, o_qg, o_kg,
    iq, ik, iv, idt, tq, tk, tv, td,
    qbuf, kbuf, vbuf, dbuf, knb, dka, dva, gq, gk, gv, gsum, dpbuf, sqbuf,
    fs, fr, bs, br, ls, gs, gr, ins,
):
    me = lax.axis_index("seq")
    my_dp = lax.axis_index("dp")
    img, txt, text = iq.shape[0], tq.shape[0], tk.shape[0]
    block = img + txt
    image = img * n
    others = partners(me, n)

    def col(owner, h):
        return pl.ds(pl.multiple_of((owner * heads + h) * HEAD_DIM, HEAD_DIM), HEAD_DIM)

    def rows(start, size, unit):
        return pl.ds(pl.multiple_of(start, unit), size)

    loads = [
        pltpu.make_async_copy(src, dst, ins.at[i])
        for i, (src, dst) in enumerate(
            zip(
                (h_iq, h_ik, h_iv, h_idt, h_tq, h_td, h_tk, h_tv),
                (iq, ik, iv, idt, tq, td, tk, tv),
            )
        )
    ]
    for load in loads:
        load.start()
    barrier = pltpu.get_barrier_semaphore()
    for other in others:
        pl.semaphore_signal(barrier, inc=1, device_id={"seq": other}, device_id_type=MESH)

    def greet(step, carry):
        pl.semaphore_signal(
            barrier, inc=1, device_id={"dp": lax.rem(my_dp + step, dp)}, device_id_type=MESH
        )
        return carry

    lax.fori_loop(1, dp, greet, 0)
    pl.semaphore_wait(barrier, n - 1 + dp - 1)
    for load in loads:
        load.wait()

    def forward_parts(h, source):
        return (
            (iq, qbuf.at[h, rows(source * block, img, 16)]),
            (ik, kbuf.at[h, rows(source * img, img, 16)]),
            (iv, vbuf.at[h, rows(source * img, img, 16)]),
            (idt, dbuf.at[h, rows(source * block, img, 16)]),
            (tq, qbuf.at[h, rows(source * block + img, txt, 16)]),
            (td, dbuf.at[h, rows(source * block + img, txt, 16)]),
        )

    def forward_copy(part, h, source, target):
        src, dst = forward_parts(h, source)[part]
        return pltpu.make_async_remote_copy(
            src_ref=src.at[:, col(target, h)], dst_ref=dst,
            send_sem=fs.at[part, h, target], recv_sem=fr.at[part, h, source],
            device_id={"seq": target}, device_id_type=MESH,
        )

    def send_head(h, carry):
        for other in others:
            for part in range(6):
                forward_copy(part, h, me, other).start()
        return carry

    lax.fori_loop(0, heads, send_head, 0)

    def own_head(h, carry):
        for src, dst in forward_parts(h, me):
            dst[...] = src[:, col(me, h)]
        kbuf[h, image:image + text] = tk[:, col(me, h)]
        vbuf[h, image:image + text] = tv[:, col(me, h)]
        return carry

    lax.fori_loop(0, heads, own_head, 0)
    gsum[...] = jnp.zeros_like(gsum)

    def back_parts(h, target):
        return (
            (gq.at[h, rows(target * block, img, 16)], o_iq),
            (gk.at[h, rows(target * img, img, 16)], o_ik),
            (gv.at[h, rows(target * img, img, 16)], o_iv),
            (gq.at[h, rows(target * block + img, txt, 16)], o_tq),
            (gk.at[h, rows(image + target * txt, txt, 16)], o_tk),
            (gv.at[h, rows(image + target * txt, txt, 16)], o_tv),
        )

    def back_copy(part, h, source, target):
        src, dst = back_parts(h, target)[part]
        return pltpu.make_async_remote_copy(
            src_ref=src, dst_ref=dst.at[:, col(source, h)],
            send_sem=bs.at[part, h, target], recv_sem=br.at[part, h, source],
            device_id={"seq": target}, device_id_type=MESH,
        )

    qg = q_gain[...]
    kg = k_gain[...]
    scale = HEAD_DIM ** (-0.5)

    def head(h, carry):
        for other in others:
            for part in range(6):
                forward_copy(part, h, other, me).wait_recv()
        key_src = kbuf[h].astype(F32)
        key_inv = inverse_rms(key_src)
        knb[...] = (key_src * key_inv * kg).astype(BF16)
        dka[...] = jnp.zeros_like(dka)
        dva[...] = jnp.zeros_like(dva)

        def one_block(j, inner):
            here = rows(j * block, block, 16)
            query_src = qbuf[h, here].astype(F32)
            query_inv = inverse_rms(query_src)
            qn = (query_src * query_inv * qg).astype(BF16)
            kn = knb[...]
            value = vbuf[h]
            dout = dbuf[h, here]
            scores = dot(qn, kn, (1, 1)) * scale
            exps = jnp.exp(scores - jnp.max(scores, axis=-1, keepdims=True))
            prob = exps * (1.0 / jnp.sum(exps, axis=-1, keepdims=True))
            prob_b = prob.astype(BF16)
            output = dot(prob_b, value, (1, 0)).astype(BF16)
            dprob = dot(dout, value, (1, 1))
            delta = jnp.sum(dout.astype(F32) * output.astype(F32), axis=-1, keepdims=True)
            dscore = (prob * (dprob - delta) * scale).astype(BF16)
            dqn = dot(dscore, kn, (1, 0))
            dka[...] += dot(dscore, qn, (0, 0)).astype(BF16).astype(F32)
            dva[...] += dot(prob_b, dout, (0, 0)).astype(BF16).astype(F32)
            dq, term = norm_back(query_src, query_inv, qg, dqn)
            gq[h, here] = dq.astype(BF16)
            gsum[0:1, :] += jnp.sum(term, axis=0, keepdims=True)
            return inner

        lax.fori_loop(0, n, one_block, 0)
        gv[h] = dva[...].astype(BF16)
        dk, term = norm_back(key_src, key_inv, kg, dka[...])
        gk[h] = dk.astype(BF16)
        gsum[1:2, :] += jnp.sum(term, axis=0, keepdims=True)
        for other in others:
            for part in range(6):
                back_copy(part, h, me, other).start()
        for part, (src, dst) in enumerate(back_parts(h, me)):
            pltpu.make_async_copy(src, dst.at[:, col(me, h)], ls.at[part, h]).start()
        return carry

    lax.fori_loop(0, heads, head, 0)

    dpbuf[my_dp] = gsum[...]

    def dp_copy(target):
        return pltpu.make_async_remote_copy(
            src_ref=dpbuf.at[my_dp], dst_ref=dpbuf.at[my_dp], send_sem=gs.at[0], recv_sem=gr.at[0],
            device_id={"dp": target}, device_id_type=MESH,
        )

    def dp_send(step, carry):
        dp_copy(lax.rem(my_dp + step, dp)).start()
        return carry

    lax.fori_loop(1, dp, dp_send, 0)
    rest = dpbuf.at[pl.ds(0, dp - 1)]
    pltpu.make_async_copy(rest, rest, gr.at[0]).wait()
    pltpu.make_async_copy(rest, rest, gs.at[0]).wait()
    sqbuf[me] = jnp.sum(dpbuf[...], axis=0)
    for other in others:
        pltpu.make_async_remote_copy(
            src_ref=sqbuf.at[me], dst_ref=sqbuf.at[me], send_sem=gs.at[1], recv_sem=gr.at[1],
            device_id={"seq": other}, device_id_type=MESH,
        ).start()

    def drain(h, carry):
        for part, (src, dst) in enumerate(back_parts(h, me)):
            pltpu.make_async_copy(src, dst.at[:, col(me, h)], ls.at[part, h]).wait()
        for other in others:
            for part in range(6):
                forward_copy(part, h, me, other).wait_send()
                back_copy(part, h, me, other).wait_send()
                back_copy(part, h, other, me).wait_recv()
        return carry

    lax.fori_loop(0, heads, drain, 0)
    rest = sqbuf.at[pl.ds(0, n - 1)]
    pltpu.make_async_copy(rest, rest, gr.at[1]).wait()
    pltpu.make_async_copy(rest, rest, gs.at[1]).wait()
    total = jnp.sum(sqbuf[...], axis=0)
    o_qg[...] = total[0:1]
    o_kg[...] = total[1:2]


def hand_on(*refs):
    count = (len(refs) - 2) // 3
    sources, results, held = refs[:count], refs[count:2 * count], refs[2 * count:3 * count]
    in_sem, out_sem = refs[3 * count:]
    loads = [pltpu.make_async_copy(a, b, in_sem.at[i]) for i, (a, b) in enumerate(zip(sources, held))]
    stores = [pltpu.make_async_copy(a, b, out_sem.at[i]) for i, (a, b) in enumerate(zip(held, results))]
    for load in loads:
        load.start()
    for load, store in zip(loads, stores):
        load.wait()
        store.start()
    for store in stores:
        store.wait()


def local(n, dp, iq, ik, iv, idt, tq, tk, tv, td, q_gain, k_gain):
    img, width = iq.shape[1:]
    txt, text = tq.shape[1], tk.shape[1]
    heads = width // HEAD_DIM // n
    keys = img * n + text
    queries = (img + txt) * n
    vmem = pl.BlockSpec(memory_space=pltpu.VMEM)
    hbm = pl.BlockSpec(memory_space=pl.ANY)
    out = pl.pallas_call(
        functools.partial(kernel, n, dp, heads),
        out_shape=(
            jax.ShapeDtypeStruct((img, width), BF16),
            jax.ShapeDtypeStruct((img, width), BF16),
            jax.ShapeDtypeStruct((img, width), BF16),
            jax.ShapeDtypeStruct((txt, width), BF16),
            jax.ShapeDtypeStruct((txt, width), BF16),
            jax.ShapeDtypeStruct((txt, width), BF16),
            jax.ShapeDtypeStruct((1, HEAD_DIM), F32),
            jax.ShapeDtypeStruct((1, HEAD_DIM), F32),
        ),
        in_specs=[hbm] * 8 + [vmem] * 2,
        out_specs=(hbm,) * 6 + (vmem,) * 2,
        scratch_shapes=[
            pltpu.VMEM((img, width), BF16),
            pltpu.VMEM((img, width), BF16),
            pltpu.VMEM((img, width), BF16),
            pltpu.VMEM((img, width), BF16),
            pltpu.VMEM((txt, width), BF16),
            pltpu.VMEM((text, width), BF16),
            pltpu.VMEM((text, width), BF16),
            pltpu.VMEM((txt, width), BF16),
            pltpu.VMEM((heads, queries, HEAD_DIM), BF16),
            pltpu.VMEM((heads, keys, HEAD_DIM), BF16),
            pltpu.VMEM((heads, keys, HEAD_DIM), BF16),
            pltpu.VMEM((heads, queries, HEAD_DIM), BF16),
            pltpu.VMEM((keys, HEAD_DIM), BF16),
            pltpu.VMEM((keys, HEAD_DIM), F32),
            pltpu.VMEM((keys, HEAD_DIM), F32),
            pltpu.VMEM((heads, queries, HEAD_DIM), BF16),
            pltpu.VMEM((heads, keys, HEAD_DIM), BF16),
            pltpu.VMEM((heads, keys, HEAD_DIM), BF16),
            pltpu.VMEM((2, HEAD_DIM), F32),
            pltpu.VMEM((dp, 2, HEAD_DIM), F32),
            pltpu.VMEM((n, 2, HEAD_DIM), F32),
            pltpu.SemaphoreType.DMA((6, heads, n)),
            pltpu.SemaphoreType.DMA((6, heads, n)),
            pltpu.SemaphoreType.DMA((6, heads, n)),
            pltpu.SemaphoreType.DMA((6, heads, n)),
            pltpu.SemaphoreType.DMA((6, heads)),
            pltpu.SemaphoreType.DMA((2,)),
            pltpu.SemaphoreType.DMA((2,)),
            pltpu.SemaphoreType.DMA((8,)),
        ],
        compiler_params=pltpu.CompilerParams(collective_id=0, has_side_effects=True),
    )(
        iq[0], ik[0], iv[0], idt[0], tq[0], tk[0], tv[0], td[0],
        q_gain.reshape(1, HEAD_DIM), k_gain.reshape(1, HEAD_DIM),
    )
    final = pl.pallas_call(
        hand_on,
        out_shape=tuple(jax.ShapeDtypeStruct(a.shape, a.dtype) for a in out),
        in_specs=[hbm] * 8,
        out_specs=(hbm,) * 8,
        scratch_shapes=[pltpu.VMEM(a.shape, a.dtype) for a in out]
        + [pltpu.SemaphoreType.DMA((8,)), pltpu.SemaphoreType.DMA((8,))],
    )(*out)
    return (*(grad[None] for grad in final[:6]), final[6][0], final[7][0])


def solution(mesh):
    split = P("dp", "seq", None)
    whole = P("dp", None, None)
    return jax.shard_map(
        functools.partial(local, mesh.shape["seq"], mesh.shape["dp"]),
        mesh=mesh,
        in_specs=(split, split, split, split, split, whole, whole, split, P(), P()),
        out_specs=(split,) * 6 + (P(), P()),
        check_vma=False,
    )
```

```python
import functools

import jax
import jax.numpy as jnp
from jax import lax
from jax.experimental import pallas as pl
from jax.experimental.pallas import tpu as pltpu
from jax.sharding import PartitionSpec as P

MESH = pl.DeviceIdType.MESH
HEAD_DIM = 128
EPSILON = 1e-06
F32 = jnp.float32
BF16 = jnp.bfloat16


def dot(a, b, contract):
    return lax.dot_general(a, b, ((contract[:1], contract[1:]), ((), ())), preferred_element_type=F32)


def inverse_rms(values):
    return lax.rsqrt(jnp.mean(values * values, axis=-1, keepdims=True) + EPSILON)


def norm_back(values, inverse, gain, upstream):
    unit = values * inverse
    lifted = upstream * gain
    mean = jnp.mean(lifted * unit, axis=-1, keepdims=True)
    return inverse * (lifted - unit * mean), upstream * unit


def partners(me, n):
    if n == 4:
        return [lax.rem(me + 2, n), 3 - me, me + 1 - 2 * lax.rem(me, 2)]
    return [lax.rem(me + step, n) for step in range(1, n)]


def kernel(
    n, dp, heads,
    h_iq, h_ik, h_iv, h_idt, h_tq, h_tk, h_tv, h_td, q_gain, k_gain,
    o_iq, o_ik, o_iv, o_tq, o_tk, o_tv, o_qg, o_kg,
    iq, ik, iv, idt, tq, tk, tv, td,
    qbuf, kbuf, vbuf, dbuf, knb, dka, dva, gq, gk, gv, gsum, dpbuf, sqbuf,
    fs, fr, bs, br, ls, gs, gr, ins,
):
    me = lax.axis_index("seq")
    my_dp = lax.axis_index("dp")
    img, txt, text = iq.shape[0], tq.shape[0], tk.shape[0]
    block = img + txt
    image = img * n
    others = partners(me, n)

    def col(owner, h):
        return pl.ds(pl.multiple_of((owner * heads + h) * HEAD_DIM, HEAD_DIM), HEAD_DIM)

    def rows(start, size, unit):
        return pl.ds(pl.multiple_of(start, unit), size)

    loads = [
        pltpu.make_async_copy(src, dst, ins.at[i])
        for i, (src, dst) in enumerate(
            zip(
                (h_iq, h_ik, h_iv, h_idt, h_tq, h_td, h_tk, h_tv),
                (iq, ik, iv, idt, tq, td, tk, tv),
            )
        )
    ]
    for load in loads:
        load.start()
    barrier = pltpu.get_barrier_semaphore()
    for other in others:
        pl.semaphore_signal(barrier, inc=1, device_id={"seq": other}, device_id_type=MESH)

    def greet(step, carry):
        pl.semaphore_signal(
            barrier, inc=1, device_id={"dp": lax.rem(my_dp + step, dp)}, device_id_type=MESH
        )
        return carry

    lax.fori_loop(1, dp, greet, 0)
    pl.semaphore_wait(barrier, n - 1 + dp - 1)
    for load in loads:
        load.wait()

    def forward_parts(h, source):
        return (
            (iq, qbuf.at[h, rows(source * block, img, 16)]),
            (ik, kbuf.at[h, rows(source * img, img, 16)]),
            (iv, vbuf.at[h, rows(source * img, img, 16)]),
            (idt, dbuf.at[h, rows(source * block, img, 16)]),
            (tq, qbuf.at[h, rows(source * block + img, txt, 16)]),
            (td, dbuf.at[h, rows(source * block + img, txt, 16)]),
        )

    def forward_copy(part, h, source, target):
        src, dst = forward_parts(h, source)[part]
        return pltpu.make_async_remote_copy(
            src_ref=src.at[:, col(target, h)], dst_ref=dst,
            send_sem=fs.at[part, h, target], recv_sem=fr.at[part, h, source],
            device_id={"seq": target}, device_id_type=MESH,
        )

    def send_head(h, carry):
        for other in others:
            for part in range(6):
                forward_copy(part, h, me, other).start()
        return carry

    lax.fori_loop(0, heads, send_head, 0)

    def own_head(h, carry):
        for src, dst in forward_parts(h, me):
            dst[...] = src[:, col(me, h)]
        kbuf[h, image:image + text] = tk[:, col(me, h)]
        vbuf[h, image:image + text] = tv[:, col(me, h)]
        return carry

    lax.fori_loop(0, heads, own_head, 0)
    gsum[...] = jnp.zeros_like(gsum)

    def back_parts(h, target):
        return (
            (gq.at[h, rows(target * block, img, 16)], o_iq),
            (gk.at[h, rows(target * img, img, 16)], o_ik),
            (gv.at[h, rows(target * img, img, 16)], o_iv),
            (gq.at[h, rows(target * block + img, txt, 16)], o_tq),
            (gk.at[h, rows(image + target * txt, txt, 16)], o_tk),
            (gv.at[h, rows(image + target * txt, txt, 16)], o_tv),
        )

    def back_copy(part, h, source, target):
        src, dst = back_parts(h, target)[part]
        return pltpu.make_async_remote_copy(
            src_ref=src, dst_ref=dst.at[:, col(source, h)],
            send_sem=bs.at[part, h, target], recv_sem=br.at[part, h, source],
            device_id={"seq": target}, device_id_type=MESH,
        )

    def send_back(h):
        for other in others:
            for part in range(6):
                back_copy(part, h, me, other).start()
        for part, (src, dst) in enumerate(back_parts(h, me)):
            pltpu.make_async_copy(src, dst.at[:, col(me, h)], ls.at[part, h]).start()

    qg = q_gain[...]
    kg = k_gain[...]
    scale = HEAD_DIM ** (-0.5)

    def head(h, carry):
        for other in others:
            for part in range(6):
                forward_copy(part, h, other, me).wait_recv()
        key_src = kbuf[h].astype(F32)
        key_inv = inverse_rms(key_src)
        knb[...] = (key_src * key_inv * kg).astype(BF16)
        dka[...] = jnp.zeros_like(dka)
        dva[...] = jnp.zeros_like(dva)

        def one_block(j, inner):
            here = rows(j * block, block, 16)
            query_src = qbuf[h, here].astype(F32)
            query_inv = inverse_rms(query_src)
            qn = (query_src * query_inv * qg).astype(BF16)
            kn = knb[...]
            value = vbuf[h]
            dout = dbuf[h, here]
            scores = dot(qn, kn, (1, 1)) * scale
            exps = jnp.exp(scores - jnp.max(scores, axis=-1, keepdims=True))
            prob = exps * (1.0 / jnp.sum(exps, axis=-1, keepdims=True))
            prob_b = prob.astype(BF16)
            output = dot(prob_b, value, (1, 0)).astype(BF16)
            dprob = dot(dout, value, (1, 1))
            delta = jnp.sum(dout.astype(F32) * output.astype(F32), axis=-1, keepdims=True)
            dscore = (prob * (dprob - delta) * scale).astype(BF16)
            dqn = dot(dscore, kn, (1, 0))
            dka[...] += dot(dscore, qn, (0, 0)).astype(BF16).astype(F32)
            dva[...] += dot(prob_b, dout, (0, 0)).astype(BF16).astype(F32)
            dq, term = norm_back(query_src, query_inv, qg, dqn)
            gq[h, here] = dq.astype(BF16)
            gsum[0:1, :] += jnp.sum(term, axis=0, keepdims=True)
            return inner

        lax.fori_loop(0, n, one_block, 0)
        gv[h] = dva[...].astype(BF16)
        dk, term = norm_back(key_src, key_inv, kg, dka[...])
        gk[h] = dk.astype(BF16)
        gsum[1:2, :] += jnp.sum(term, axis=0, keepdims=True)

        @pl.when(h < heads - 1)
        def _():
            send_back(h)

        return carry

    lax.fori_loop(0, heads, head, 0)

    dpbuf[my_dp] = gsum[...]

    def dp_copy(target):
        return pltpu.make_async_remote_copy(
            src_ref=dpbuf.at[my_dp], dst_ref=dpbuf.at[my_dp], send_sem=gs.at[0], recv_sem=gr.at[0],
            device_id={"dp": target}, device_id_type=MESH,
        )

    def dp_send(step, carry):
        dp_copy(lax.rem(my_dp + step, dp)).start()
        return carry

    lax.fori_loop(1, dp, dp_send, 0)
    rest = dpbuf.at[pl.ds(0, dp - 1)]
    pltpu.make_async_copy(rest, rest, gr.at[0]).wait()
    pltpu.make_async_copy(rest, rest, gs.at[0]).wait()
    sqbuf[me] = jnp.sum(dpbuf[...], axis=0)
    for other in others:
        pltpu.make_async_remote_copy(
            src_ref=sqbuf.at[me], dst_ref=sqbuf.at[me], send_sem=gs.at[1], recv_sem=gr.at[1],
            device_id={"seq": other}, device_id_type=MESH,
        ).start()
    send_back(heads - 1)

    def drain(h, carry):
        for part, (src, dst) in enumerate(back_parts(h, me)):
            pltpu.make_async_copy(src, dst.at[:, col(me, h)], ls.at[part, h]).wait()
        for other in others:
            for part in range(6):
                forward_copy(part, h, me, other).wait_send()
                back_copy(part, h, me, other).wait_send()
                back_copy(part, h, other, me).wait_recv()
        return carry

    lax.fori_loop(0, heads, drain, 0)
    rest = sqbuf.at[pl.ds(0, n - 1)]
    pltpu.make_async_copy(rest, rest, gr.at[1]).wait()
    pltpu.make_async_copy(rest, rest, gs.at[1]).wait()
    total = jnp.sum(sqbuf[...], axis=0)
    o_qg[...] = total[0:1]
    o_kg[...] = total[1:2]


def hand_on(*refs):
    count = (len(refs) - 2) // 3
    sources, results, held = refs[:count], refs[count:2 * count], refs[2 * count:3 * count]
    in_sem, out_sem = refs[3 * count:]
    loads = [pltpu.make_async_copy(a, b, in_sem.at[i]) for i, (a, b) in enumerate(zip(sources, held))]
    stores = [pltpu.make_async_copy(a, b, out_sem.at[i]) for i, (a, b) in enumerate(zip(held, results))]
    for load in loads:
        load.start()
    for load, store in zip(loads, stores):
        load.wait()
        store.start()
    for store in stores:
        store.wait()


def local(n, dp, iq, ik, iv, idt, tq, tk, tv, td, q_gain, k_gain):
    img, width = iq.shape[1:]
    txt, text = tq.shape[1], tk.shape[1]
    heads = width // HEAD_DIM // n
    keys = img * n + text
    queries = (img + txt) * n
    vmem = pl.BlockSpec(memory_space=pltpu.VMEM)
    hbm = pl.BlockSpec(memory_space=pl.ANY)
    out = pl.pallas_call(
        functools.partial(kernel, n, dp, heads),
        out_shape=(
            jax.ShapeDtypeStruct((img, width), BF16),
            jax.ShapeDtypeStruct((img, width), BF16),
            jax.ShapeDtypeStruct((img, width), BF16),
            jax.ShapeDtypeStruct((txt, width), BF16),
            jax.ShapeDtypeStruct((txt, width), BF16),
            jax.ShapeDtypeStruct((txt, width), BF16),
            jax.ShapeDtypeStruct((1, HEAD_DIM), F32),
            jax.ShapeDtypeStruct((1, HEAD_DIM), F32),
        ),
        in_specs=[hbm] * 8 + [vmem] * 2,
        out_specs=(hbm,) * 6 + (vmem,) * 2,
        scratch_shapes=[
            pltpu.VMEM((img, width), BF16),
            pltpu.VMEM((img, width), BF16),
            pltpu.VMEM((img, width), BF16),
            pltpu.VMEM((img, width), BF16),
            pltpu.VMEM((txt, width), BF16),
            pltpu.VMEM((text, width), BF16),
            pltpu.VMEM((text, width), BF16),
            pltpu.VMEM((txt, width), BF16),
            pltpu.VMEM((heads, queries, HEAD_DIM), BF16),
            pltpu.VMEM((heads, keys, HEAD_DIM), BF16),
            pltpu.VMEM((heads, keys, HEAD_DIM), BF16),
            pltpu.VMEM((heads, queries, HEAD_DIM), BF16),
            pltpu.VMEM((keys, HEAD_DIM), BF16),
            pltpu.VMEM((keys, HEAD_DIM), F32),
            pltpu.VMEM((keys, HEAD_DIM), F32),
            pltpu.VMEM((heads, queries, HEAD_DIM), BF16),
            pltpu.VMEM((heads, keys, HEAD_DIM), BF16),
            pltpu.VMEM((heads, keys, HEAD_DIM), BF16),
            pltpu.VMEM((2, HEAD_DIM), F32),
            pltpu.VMEM((dp, 2, HEAD_DIM), F32),
            pltpu.VMEM((n, 2, HEAD_DIM), F32),
            pltpu.SemaphoreType.DMA((6, heads, n)),
            pltpu.SemaphoreType.DMA((6, heads, n)),
            pltpu.SemaphoreType.DMA((6, heads, n)),
            pltpu.SemaphoreType.DMA((6, heads, n)),
            pltpu.SemaphoreType.DMA((6, heads)),
            pltpu.SemaphoreType.DMA((2,)),
            pltpu.SemaphoreType.DMA((2,)),
            pltpu.SemaphoreType.DMA((8,)),
        ],
        compiler_params=pltpu.CompilerParams(collective_id=0, has_side_effects=True),
    )(
        iq[0], ik[0], iv[0], idt[0], tq[0], tk[0], tv[0], td[0],
        q_gain.reshape(1, HEAD_DIM), k_gain.reshape(1, HEAD_DIM),
    )
    final = pl.pallas_call(
        hand_on,
        out_shape=tuple(jax.ShapeDtypeStruct(a.shape, a.dtype) for a in out),
        in_specs=[hbm] * 8,
        out_specs=(hbm,) * 8,
        scratch_shapes=[pltpu.VMEM(a.shape, a.dtype) for a in out]
        + [pltpu.SemaphoreType.DMA((8,)), pltpu.SemaphoreType.DMA((8,))],
    )(*out)
    return (*(grad[None] for grad in final[:6]), final[6][0], final[7][0])


def solution(mesh):
    split = P("dp", "seq", None)
    whole = P("dp", None, None)
    return jax.shard_map(
        functools.partial(local, mesh.shape["seq"], mesh.shape["dp"]),
        mesh=mesh,
        in_specs=(split, split, split, split, split, whole, whole, split, P(), P()),
        out_specs=(split,) * 6 + (P(), P()),
        check_vma=False,
    )
```
